32 devices in a mesh: group: 2 (over y), hi: 4 (over z), lo: 2 (over x), cuts: 2 (over core).
Axes of the slice: x: 2, y: 2, z: 4, core: 2. Of those that a mesh axis runs over, the one named last changes fastest.
Arguments:
- state_block: float32 [8, 2, 131072], P(('group', 'hi'), 'lo'), parts along dimension 0, may hold values from -6 to 6
- gate_table: float32 [4, 256, 256], replicated, may hold values from -0.375 to 0.375
- closing_table: float32 [4, 2, 2, 256], replicated, may hold values from -1 to 1
- slice_edges: int32 [8, 3], P(('group', 'cuts')), parts along dimension 0, may hold values from 0 to 3
- bit_orders: int32 [2, 8], replicated, may hold values from 0 to 7, each once within a row
Outputs:
- amplitudes: float32 [8, 2, 65536], P(('group', 'hi'), 'lo', 'cuts'), parts along dimension 0
The draws below stay inside these ranges and needn't reach their ends.
There are 2 independent parts, one for each index of `group`. The reference program is written for one: setup_inputs(seed, part) draws one part's arguments, and reference() takes and returns one part's arrays. A program takes and returns all parts, laid end to end along the dimension named above; an argument that names none is the same for every part. Nothing has to cross between parts.
Inputs may be any that keep to these rules, and one draw needn't show every extreme that they name: `bit_orders`: each row is a permutation of 0 to 7.
All inputs are finite; a program needn't handle non-finite values.
Results may differ from the reference program's by a relative error of at most 0.0001.
Values sent between devices are 32-bit elements; how exact they have to be, the bound alone decides.
No kernel may reach another device: no remote copies, remote signals or barrier semaphores. Data moves between devices by JAX's collectives and lax.ppermute only.
A program may use at most 64 MiB of HBM per device.

```python
import jax
import jax.numpy as jnp
from jax import lax

BITS = 8
GATE = 256
CLOSED = 2
MIDDLE = 1
EDGES = 4
SLICES = 4
HI_SPAN = 64
LO_SPAN = 128
LOCAL = 131072
AMPS = 65536
N_HI = 4
N_LO = 2


def plant(entries, key, least, high):
    shape = entries.shape
    spot = [jax.random.randint(jax.random.fold_in(key, axis), (), 0, shape[axis]) for axis in range(len(shape))]
    entries = entries.at[tuple(spot)].set(least)
    longest = shape.index(max(shape))
    spot[longest] = (spot[longest] + 1) % shape[longest]
    return entries.at[tuple(spot)].set(high)


def block_levels(stream_key, extent, cuts, low, high):
    loudness = 1.0
    for position, parts in cuts:
        heights = jax.random.uniform(jax.random.fold_in(jax.random.fold_in(stream_key, 6), position), (parts,), jnp.float32, low / len(cuts), high / len(cuts))
        loudness = loudness * jnp.repeat(jnp.exp(heights), extent[position] // parts).reshape((-1,) + (1,) * (len(extent) - 1 - position))
    return loudness


def gaussian(own_key, extent, scale, limit, cuts=(), kind=jnp.bfloat16):
    drawn = scale * jax.random.normal(own_key, extent, jnp.float32)
    if cuts:
        drawn = drawn * block_levels(own_key, extent, cuts, -0.22, 0.18)
    return jnp.clip(drawn, -limit, limit).astype(kind)


def setup_inputs(seed: int = 0, part: int = 0) -> dict:
    splits = jax.random.split(jax.random.key(seed), 6)
    own_keys = jax.random.split(jax.random.fold_in(splits[5], part), 6)
    return {
        "state_block": gaussian(own_keys[0], (N_HI, N_LO, LOCAL), 1.0, 6.0, ((0, 4), (1, 2)), jnp.float32),
        "gate_table": gaussian(splits[1], (EDGES, GATE, GATE), GATE ** -0.5, 0.375, (), jnp.float32),
        "closing_table": jnp.clip(jax.random.uniform(splits[2], (EDGES, 2, CLOSED, GATE), jnp.float32, -1.0, 1.0), -1.0, 1.0),
        "slice_edges": plant(jax.random.randint(own_keys[3], (SLICES, 3), 0, EDGES), jax.random.fold_in(own_keys[3], 1), 0, EDGES - 1).astype(jnp.int32),
        "bit_orders": jax.vmap(lambda own: jax.random.permutation(own, BITS))(jax.random.split(splits[4], 2)).reshape((2, BITS)).astype(jnp.int32),
    }


def permuted(gate, order):
    rows = jnp.arange(GATE, dtype=jnp.int32)
    picked = (rows[:, None] >> order[None, :].astype(jnp.int32)) & 1
    weights = jnp.left_shift(jnp.ones((BITS,), jnp.int32), jnp.arange(BITS, dtype=jnp.int32))
    source = jnp.sum(picked * weights[None, :], axis=1).astype(jnp.int32)
    return jnp.take(gate, source, axis=0)


def reference(state_block, gate_table, closing_table, slice_edges, bit_orders):
    tensor = state_block.reshape(N_HI, N_LO, HI_SPAN, N_HI, CLOSED, MIDDLE, N_LO, LO_SPAN)
    total = jnp.zeros((N_HI, N_LO, AMPS), jnp.float32)
    for slice_index in range(SLICES):
        chosen = slice_edges[slice_index]
        first = permuted(gate_table[chosen[0]], bit_orders[0]).reshape(HI_SPAN, N_HI, HI_SPAN, N_HI)
        second = permuted(gate_table[chosen[1]], bit_orders[1]).reshape(N_LO, LO_SPAN, N_LO, LO_SPAN)
        front = closing_table[chosen[2], 0].reshape(CLOSED, HI_SPAN, N_HI)
        rear = closing_table[chosen[2], 1].reshape(CLOSED, N_LO, LO_SPAN)
        section_one = jnp.einsum('phPH,hlpbzmeq->HlPbzmeq', first, tensor, precision=lax.Precision.HIGHEST)
        weight_one = jnp.transpose(front, (2, 1, 0))
        section_one = section_one * weight_one[:, None, :, None, :, None, None, None]
        section_two = jnp.einsum('lqLQ,hlpbzmeq->hLpbzmeQ', second, section_one, precision=lax.Precision.HIGHEST)
        closed = jnp.einsum('zLQ,hLpbzmeQ->hLpbmeQ', rear, section_two, precision=lax.Precision.HIGHEST)
        total = total + closed.reshape(N_HI, N_LO, AMPS)
    return total
```

```python
import jax
import jax.numpy as jnp
from jax import lax
from jax.sharding import PartitionSpec as P


def swap(value, axis, offset):
    if offset == 0:
        return value
    return lax.ppermute(value, axis, [(i, i ^ offset) for i in range(lax.axis_size(axis))])


def sources(order, wanted):
    total = jnp.zeros_like(wanted)
    for i in range(order.shape[0]):
        total = total + (((wanted >> order[i]) & 1) << i)
    return total


def local(state_block, gate_table, closing_table, slice_edges, bit_orders):
    n_hi, n_lo, n_cuts = lax.axis_size("hi"), lax.axis_size("lo"), lax.axis_size("cuts")
    h, l, c = lax.axis_index("hi"), lax.axis_index("lo"), lax.axis_index("cuts")
    gate = gate_table.shape[1]
    closed = closing_table.shape[2]
    span_hi, span_lo = gate // n_hi, gate // n_lo
    middle = state_block.shape[2] // (gate * gate * closed)
    part_e = n_lo // n_cuts
    part_p = span_hi // n_cuts
    edges = jnp.concatenate([swap(slice_edges, "cuts", k) for k in range(n_cuts)])
    slices = edges.shape[0]

    view = state_block.reshape(span_hi, n_hi, closed, middle, n_cuts, part_e, span_lo)
    mine = lax.dynamic_index_in_dim(view, c, 4, keepdims=False)
    parts = []
    for d in range(n_hi):
        piece = lax.dynamic_index_in_dim(mine, h ^ d, 1, keepdims=False)
        parts.append(swap(piece, "hi", d))
    data = jnp.stack(parts).reshape(gate, closed, middle * part_e, span_lo)

    along = jnp.arange(gate, dtype=jnp.int32)
    in_rows = (along % span_hi) * n_hi + (h ^ (along // span_hi))
    out_p = (c ^ (along // part_p % n_cuts)) * part_p + along % part_p
    out_rows = out_p * n_hi + (h ^ (along // span_hi))
    in_cols = l * span_lo + jnp.arange(span_lo, dtype=jnp.int32)
    out_cols = (l ^ (along // span_lo)) * span_lo + along % span_lo
    rows_one = sources(bit_orders[0], in_rows)
    rows_two = sources(bit_orders[1], in_cols)
    firsts, seconds, fronts = [], [], []
    for s in range(slices):
        first = gate_table[edges[s, 0]]
        firsts.append(first[rows_one][:, out_rows].T)
        second = gate_table[edges[s, 1]][rows_two][:, out_cols]
        rear = closing_table[edges[s, 2], 1][:, out_cols]
        seconds.append(rear[:, None, :] * second[None])
        fronts.append(closing_table[edges[s, 2], 0][:, out_rows])
    first = jnp.stack(firsts).reshape(slices, n_hi, n_cuts, part_p, gate)
    front = jnp.stack(fronts).reshape(slices, closed, n_hi, n_cuts, part_p)
    second = jnp.stack(seconds)

    def sections(k):
        one = jnp.einsum(
            "sdpm,mzeq->sdpzeq", first[:, :, k], data, precision=lax.Precision.HIGH,
            preferred_element_type=jnp.float32,
        )
        one = one * jnp.transpose(front[:, :, :, k], (0, 2, 3, 1))[..., None, None]
        return jnp.einsum(
            "sdpzeq,szqn->depn", one, second, precision=lax.Precision.HIGH,
            preferred_element_type=jnp.float32,
        )

    others = [swap(sections(k), "cuts", k) for k in range(n_cuts)]
    both = jnp.stack(others).reshape(n_cuts, n_hi, middle * part_e, part_p, n_lo, span_lo)
    summed = sum(swap(both[:, :, :, :, k], "lo", k) for k in range(n_lo))
    out = jnp.zeros((part_p, n_hi, middle, n_cuts, part_e, span_lo), jnp.float32)
    for d in range(n_hi):
        piece = swap(summed[:, d], "hi", d).reshape(n_cuts, middle, part_e, part_p, span_lo)
        for k in range(n_cuts):
            block = jnp.transpose(piece[k], (2, 0, 1, 3))[:, None, :, None]
            out = lax.dynamic_update_slice(out, block, (0, h ^ d, 0, c ^ k, 0, 0))
    return out.reshape(1, 1, -1)


def solution(mesh):
    in_specs = (P(("group", "hi"), "lo", None), P(), P(), P(("group", "cuts"), None), P())
    out_specs = P(("group", "hi"), "lo", "cuts")
    return jax.shard_map(local, mesh=mesh, in_specs=in_specs, out_specs=out_specs, check_vma=False)
```

```python
import functools

import jax
import jax.numpy as jnp
from jax import lax
from jax.experimental import pallas as pl
from jax.experimental.pallas import tpu as pltpu
from jax.sharding import PartitionSpec as P

F32, BF16 = jnp.float32, jnp.bfloat16
VMEM = pl.BlockSpec(memory_space=pltpu.VMEM)
SMEM = pl.BlockSpec(memory_space=pltpu.SMEM)


def swap(value, axis, offset):
    if offset == 0:
        return value
    return lax.ppermute(value, axis, [(i, i ^ offset) for i in range(lax.axis_size(axis))])


def sources(order, wanted):
    total = jnp.zeros_like(wanted)
    for i in range(order.shape[0]):
        total = total + (((wanted >> order[i]) & 1) << i)
    return total


def general(state_block, gate_table, closing_table, edges, bit_orders):
    n_hi, n_lo, n_cuts = lax.axis_size("hi"), lax.axis_size("lo"), lax.axis_size("cuts")
    h, l, c = lax.axis_index("hi"), lax.axis_index("lo"), lax.axis_index("cuts")
    gate = gate_table.shape[1]
    closed = closing_table.shape[2]
    span_hi, span_lo = gate // n_hi, gate // n_lo
    middle = state_block.shape[2] // (gate * gate * closed)
    part_e = n_lo // n_cuts
    part_p = span_hi // n_cuts
    slices = edges.shape[0]

    view = state_block.reshape(span_hi, n_hi, closed, middle, n_cuts, part_e, span_lo)
    mine = lax.dynamic_index_in_dim(view, c, 4, keepdims=False)
    parts = []
    for d in range(n_hi):
        piece = lax.dynamic_index_in_dim(mine, h ^ d, 1, keepdims=False)
        parts.append(swap(piece, "hi", d))
    data = jnp.stack(parts).reshape(gate, closed, middle * part_e, span_lo)

    along = jnp.arange(gate, dtype=jnp.int32)
    in_rows = (along % span_hi) * n_hi + (h ^ (along // span_hi))
    out_p = (c ^ (along // part_p % n_cuts)) * part_p + along % part_p
    out_rows = out_p * n_hi + (h ^ (along // span_hi))
    in_cols = l * span_lo + jnp.arange(span_lo, dtype=jnp.int32)
    out_cols = (l ^ (along // span_lo)) * span_lo + along % span_lo
    rows_one = sources(bit_orders[0], in_rows)
    rows_two = sources(bit_orders[1], in_cols)
    firsts, seconds, fronts = [], [], []
    for s in range(slices):
        first = gate_table[edges[s, 0]]
        firsts.append(first[rows_one][:, out_rows].T)
        second = gate_table[edges[s, 1]][rows_two][:, out_cols]
        rear = closing_table[edges[s, 2], 1][:, out_cols]
        seconds.append(rear[:, None, :] * second[None])
        fronts.append(closing_table[edges[s, 2], 0][:, out_rows])
    first = jnp.stack(firsts).reshape(slices, n_hi, n_cuts, part_p, gate)
    front = jnp.stack(fronts).reshape(slices, closed, n_hi, n_cuts, part_p)
    second = jnp.stack(seconds)

    def sections(k):
        one = jnp.einsum(
            "sdpm,mzeq->sdpzeq", first[:, :, k], data, precision=lax.Precision.HIGH,
            preferred_element_type=F32,
        )
        one = one * jnp.transpose(front[:, :, :, k], (0, 2, 3, 1))[..., None, None]
        return jnp.einsum(
            "sdpzeq,szqn->depn", one, second, precision=lax.Precision.HIGH,
            preferred_element_type=F32,
        )

    others = [swap(sections(k), "cuts", k) for k in range(n_cuts)]
    both = jnp.stack(others).reshape(n_cuts, n_hi, middle * part_e, part_p, n_lo, span_lo)
    summed = sum(swap(both[:, :, :, :, k], "lo", k) for k in range(n_lo))
    out = jnp.zeros((part_p, n_hi, middle, n_cuts, part_e, span_lo), F32)
    for d in range(n_hi):
        piece = swap(summed[:, d], "hi", d).reshape(n_cuts, middle, part_e, part_p, span_lo)
        for k in range(n_cuts):
            block = jnp.transpose(piece[k], (2, 0, 1, 3))[:, None, :, None]
            out = lax.dynamic_update_slice(out, block, (0, h ^ d, 0, c ^ k, 0, 0))
    return out.reshape(1, 1, -1)


def split(value):
    high = value.astype(BF16)
    return high, (value - high.astype(F32)).astype(BF16)


def dot(a, b, sides=((1,), (0,))):
    return lax.dot_general(a, b, (sides, ((), ())), preferred_element_type=F32)


def pack_kernel(n_hi, closed, n_lo, place, x_ref, *pieces):
    h, c = place[0], place[2]
    span = pieces[0].shape[1]
    for d, piece in enumerate(pieces):
        for z in range(closed):
            first = ((h ^ d) * closed + z) * n_lo + c
            piece[z] = x_ref[pl.ds(first, span, stride=n_hi * closed * n_lo), :]


def gates_kernel(
    n_hi, n_cuts, place, edges, orders, gate_ref, close_ref,
    one_high, one_low, two_high, two_low, front_ref,
):
    h, l, c = place[0], place[1], place[2]
    gate = gate_ref.shape[1]
    slices, closed, span_lo = edges.shape[0], two_high.shape[1], two_high.shape[2]
    span_hi = gate // n_hi
    part_p = span_hi // n_cuts
    part = n_hi * part_p
    lane = lax.broadcasted_iota(jnp.int32, (1, gate), 1)
    row = lax.broadcasted_iota(jnp.int32, (gate, gate), 0)

    def pick(hits):
        return jnp.where(hits, 1.0, 0.0)

    wanted = (lane % span_hi) * n_hi + (h ^ (lane // span_hi))
    source = jnp.zeros_like(lane)
    target = jnp.zeros_like(lane)
    for i in range(orders.shape[1]):
        source = source + (((wanted >> orders[0, i]) & 1) << i)
        target = target + (((lane >> i) & 1) << orders[1, i])
    rows_one = pick(row == source).astype(BF16)
    p_out, h_out = lane // n_hi, lane % n_hi
    place_out = ((p_out // part_p) ^ c) * part + (h_out ^ h) * part_p + p_out % part_p
    out_one = pick(row == place_out)
    out_one_bf = out_one.astype(BF16)
    rows_two = pick(row[:span_lo] == target - l * span_lo).astype(BF16)
    out_two = pick(row == (l ^ (lane // span_lo)) * span_lo + lane % span_lo).astype(BF16)

    for s in range(slices):
        for piece, ref in zip(split(gate_ref[edges[s, 0]]), (one_high, one_low)):
            moved = dot(out_one_bf, piece, ((1,), (1,))).astype(BF16)
            moved = dot(moved, rows_one).astype(BF16)
            for k in range(n_cuts):
                ref[k, s * part : (s + 1) * part] = moved[k * part : (k + 1) * part]
        high, low = split(gate_ref[edges[s, 1]])
        picked = dot(rows_two, high) + dot(rows_two, low)
        for z in range(closed):
            front = out_one * close_ref[edges[s, 2], 0, z : z + 1]
            front = jnp.broadcast_to(jnp.sum(front, axis=1, keepdims=True), (gate, span_lo))
            for k in range(n_cuts):
                front_ref[k, s, z] = front[k * part : (k + 1) * part]
            scaled = picked * close_ref[edges[s, 2], 1, z : z + 1]
            for piece, ref in zip(split(scaled), (two_high, two_low)):
                ref[s, z] = dot(piece, out_two).astype(BF16)


def sections_kernel(k, n_data, *refs):
    pieces = refs[:n_data]
    one_high, one_low, two_high, two_low, front_ref, out_ref = refs[n_data:]
    slices, closed, part, span_lo = front_ref.shape[1:]
    data = jnp.concatenate(
        [jnp.concatenate([p[z] for z in range(closed)], axis=1) for p in pieces], axis=0
    )
    high, low = split(data)
    total = None
    for s in range(slices):
        rows = slice(s * part, (s + 1) * part)
        first_high = one_high[k, rows]
        one = dot(first_high, high) + dot(one_low[k, rows], high) + dot(first_high, low)
        one = jnp.concatenate(
            [one[:, z * span_lo : (z + 1) * span_lo] * front_ref[k, s, z] for z in range(closed)],
            axis=1,
        )
        one_h, one_l = split(one)
        second_high = two_high[s].reshape(closed * span_lo, -1)
        second_low = two_low[s].reshape(closed * span_lo, -1)
        term = dot(one_h, second_high) + dot(one_l, second_high) + dot(one_h, second_low)
        total = term if total is None else total + term
    for j in range(out_ref.shape[0]):
        out_ref[j] = total[:, j * span_lo : (j + 1) * span_lo]


def place_kernel(n_cuts, place, *refs):
    h, c = place[0], place[2]
    pieces, out_ref = refs[:-1], refs[-1]
    part_p = pieces[0].shape[1]
    step = len(pieces) * n_cuts
    for d, piece in enumerate(pieces):
        for k in range(n_cuts):
            first = (h ^ d) * n_cuts + (c ^ k)
            out_ref[pl.ds(first, part_p, stride=step), :] = piece[k]


def cost(flops, bytes_accessed):
    return pl.CostEstimate(flops=flops, bytes_accessed=bytes_accessed, transcendentals=0)


def tiled(state_block, gate_table, closing_table, edges, bit_orders):
    n_hi, n_lo, n_cuts = lax.axis_size("hi"), lax.axis_size("lo"), lax.axis_size("cuts")
    gate = gate_table.shape[1]
    closed = closing_table.shape[2]
    span_hi, span_lo = gate // n_hi, gate // n_lo
    part_p = span_hi // n_cuts
    part = n_hi * part_p
    slices = edges.shape[0]
    place = jnp.stack([lax.axis_index(name) for name in ("hi", "lo", "cuts")]).astype(jnp.int32)

    rows = state_block.reshape(-1, span_lo)
    pieces = pl.pallas_call(
        functools.partial(pack_kernel, n_hi, closed, n_lo),
        out_shape=[jax.ShapeDtypeStruct((closed, span_hi, span_lo), F32)] * n_hi,
        in_specs=[SMEM, VMEM],
        out_specs=[VMEM] * n_hi,
        cost_estimate=cost(0, 2 * rows.size * 4),
        name="pack",
    )(place, rows)
    data = [swap(piece, "hi", d) for d, piece in enumerate(pieces)]

    gates = pl.pallas_call(
        functools.partial(gates_kernel, n_hi, n_cuts),
        out_shape=[jax.ShapeDtypeStruct((n_cuts, slices * part, gate), BF16)] * 2
        + [jax.ShapeDtypeStruct((slices, closed, span_lo, gate), BF16)] * 2
        + [jax.ShapeDtypeStruct((n_cuts, slices, closed, part, span_lo), F32)],
        in_specs=[SMEM, SMEM, SMEM, VMEM, VMEM],
        out_specs=[VMEM] * 5,
        cost_estimate=cost(2_000_000_000, 4_000_000),
        name="gates",
    )(place, edges, bit_orders, gate_table, closing_table)

    def sections(k):
        return pl.pallas_call(
            functools.partial(sections_kernel, k, n_hi),
            out_shape=jax.ShapeDtypeStruct((n_lo, part, span_lo), F32),
            in_specs=[VMEM] * (n_hi + 5),
            out_specs=VMEM,
            cost_estimate=cost(800_000_000, 2_000_000),
            name=f"sections{k}",
        )(*data, *gates)

    both = [swap(sections(k), "cuts", k) for k in reversed(range(n_cuts))][::-1]
    summed = sum(swap(jnp.stack([one[j] for one in both]), "lo", j) for j in range(n_lo))
    summed = summed.reshape(n_cuts, n_hi, part_p, span_lo)
    ends = [swap(summed[:, d], "hi", d) for d in range(n_hi)]
    out = pl.pallas_call(
        functools.partial(place_kernel, n_cuts),
        out_shape=jax.ShapeDtypeStruct((part_p * n_hi * n_lo, span_lo), F32),
        in_specs=[SMEM] + [VMEM] * n_hi,
        out_specs=VMEM,
        cost_estimate=cost(0, 2 * part_p * gate * n_lo * 4),
        name="place",
    )(place, *ends)
    return out.reshape(1, 1, -1)


def local(state_block, gate_table, closing_table, slice_edges, bit_orders):
    n_hi, n_lo, n_cuts = lax.axis_size("hi"), lax.axis_size("lo"), lax.axis_size("cuts")
    gate, closed = gate_table.shape[1], closing_table.shape[2]
    edges = jnp.concatenate([swap(slice_edges, "cuts", k) for k in range(n_cuts)])
    middle = state_block.shape[2] // (gate * gate * closed)
    whole = middle == 1 and n_lo == n_cuts and gate // n_lo % 128 == 0
    whole = whole and gate // n_hi // n_cuts % 8 == 0
    plan = tiled if whole else general
    return plan(state_block, gate_table, closing_table, edges, bit_orders)


def solution(mesh):
    in_specs = (P(("group", "hi"), "lo", None), P(), P(), P(("group", "cuts"), None), P())
    out_specs = P(("group", "hi"), "lo", "cuts")
    return jax.shard_map(local, mesh=mesh, in_specs=in_specs, out_specs=out_specs, check_vma=False)
```

```python
import functools

import jax
import jax.numpy as jnp
from jax import lax
from jax.experimental import pallas as pl
from jax.experimental.pallas import tpu as pltpu
from jax.sharding import PartitionSpec as P

F32, BF16 = jnp.float32, jnp.bfloat16
VMEM = pl.BlockSpec(memory_space=pltpu.VMEM)
SMEM = pl.BlockSpec(memory_space=pltpu.SMEM)
LIMIT = pltpu.CompilerParams(vmem_limit_bytes=16 * 2**20)


def swap(value, axis, offset):
    if offset == 0:
        return value
    return lax.ppermute(value, axis, [(i, i ^ offset) for i in range(lax.axis_size(axis))])


def sources(order, wanted):
    total = jnp.zeros_like(wanted)
    for i in range(order.shape[0]):
        total = total + (((wanted >> order[i]) & 1) << i)
    return total


def general(state_block, gate_table, closing_table, edges, bit_orders):
    n_hi, n_lo, n_cuts = lax.axis_size("hi"), lax.axis_size("lo"), lax.axis_size("cuts")
    h, l, c = lax.axis_index("hi"), lax.axis_index("lo"), lax.axis_index("cuts")
    gate = gate_table.shape[1]
    closed = closing_table.shape[2]
    span_hi, span_lo = gate // n_hi, gate // n_lo
    middle = state_block.shape[2] // (gate * gate * closed)
    part_e = n_lo // n_cuts
    part_p = span_hi // n_cuts
    slices = edges.shape[0]

    view = state_block.reshape(span_hi, n_hi, closed, middle, n_cuts, part_e, span_lo)
    mine = lax.dynamic_index_in_dim(view, c, 4, keepdims=False)
    parts = []
    for d in range(n_hi):
        piece = lax.dynamic_index_in_dim(mine, h ^ d, 1, keepdims=False)
        parts.append(swap(piece, "hi", d))
    data = jnp.stack(parts).reshape(gate, closed, middle * part_e, span_lo)

    along = jnp.arange(gate, dtype=jnp.int32)
    in_rows = (along % span_hi) * n_hi + (h ^ (along // span_hi))
    out_p = (c ^ (along // part_p % n_cuts)) * part_p + along % part_p
    out_rows = out_p * n_hi + (h ^ (along // span_hi))
    in_cols = l * span_lo + jnp.arange(span_lo, dtype=jnp.int32)
    out_cols = (l ^ (along // span_lo)) * span_lo + along % span_lo
    rows_one = sources(bit_orders[0], in_rows)
    rows_two = sources(bit_orders[1], in_cols)
    firsts, seconds, fronts = [], [], []
    for s in range(slices):
        first = gate_table[edges[s, 0]]
        firsts.append(first[rows_one][:, out_rows].T)
        second = gate_table[edges[s, 1]][rows_two][:, out_cols]
        rear = closing_table[edges[s, 2], 1][:, out_cols]
        seconds.append(rear[:, None, :] * second[None])
        fronts.append(closing_table[edges[s, 2], 0][:, out_rows])
    first = jnp.stack(firsts).reshape(slices, n_hi, n_cuts, part_p, gate)
    front = jnp.stack(fronts).reshape(slices, closed, n_hi, n_cuts, part_p)
    second = jnp.stack(seconds)

    def sections(k):
        one = jnp.einsum(
            "sdpm,mzeq->sdpzeq", first[:, :, k], data, precision=lax.Precision.HIGH,
            preferred_element_type=F32,
        )
        one = one * jnp.transpose(front[:, :, :, k], (0, 2, 3, 1))[..., None, None]
        return jnp.einsum(
            "sdpzeq,szqn->depn", one, second, precision=lax.Precision.HIGH,
            preferred_element_type=F32,
        )

    others = [swap(sections(k), "cuts", k) for k in range(n_cuts)]
    both = jnp.stack(others).reshape(n_cuts, n_hi, middle * part_e, part_p, n_lo, span_lo)
    summed = sum(swap(both[:, :, :, :, k], "lo", k) for k in range(n_lo))
    out = jnp.zeros((part_p, n_hi, middle, n_cuts, part_e, span_lo), F32)
    for d in range(n_hi):
        piece = swap(summed[:, d], "hi", d).reshape(n_cuts, middle, part_e, part_p, span_lo)
        for k in range(n_cuts):
            block = jnp.transpose(piece[k], (2, 0, 1, 3))[:, None, :, None]
            out = lax.dynamic_update_slice(out, block, (0, h ^ d, 0, c ^ k, 0, 0))
    return out.reshape(1, 1, -1)


def split(value):
    high = value.astype(BF16)
    return high, (value - high.astype(F32)).astype(BF16)


def dot(a, b, sides=((1,), (0,))):
    return lax.dot_general(a, b, (sides, ((), ())), preferred_element_type=F32)


def pinned(shape, dtype=F32):
    return pltpu.VMEM(shape, dtype)


def held(value):
    return pltpu.with_memory_space_constraint(value, pltpu.VMEM)


def pack_kernel(n_hi, closed, n_lo, x_ref, *chunks):
    c = lax.axis_index("cuts")
    count, _, span = chunks[0].shape[:3]
    for t, chunk in enumerate(chunks):
        for i in range(count):
            for z in range(closed):
                first = ((t * count + i) * closed + z) * n_lo + c
                chunk[i, z] = x_ref[pl.ds(first, span, stride=n_hi * closed * n_lo), :]


def ring_order(n):
    order = [0]
    for t in range(1, n // 2):
        order += [-t, t]
    return order + [n // 2]


def gates_kernel(n_hi, n_cuts, *refs):
    edges, (orders, gate_ref, close_ref) = refs[:n_cuts], refs[n_cuts : n_cuts + 3]
    one_high, one_low, two_high, two_low, front_ref = refs[n_cuts + 3 :]
    h, l, c = (lax.axis_index(name) for name in ("hi", "lo", "cuts"))
    gate = gate_ref.shape[1]
    closed, span_lo = front_ref.shape[1], front_ref.shape[3]
    span_hi = gate // n_hi
    part_p = span_hi // n_cuts
    lane = lax.broadcasted_iota(jnp.int32, (1, gate), 1)
    row = lax.broadcasted_iota(jnp.int32, (gate, gate), 0)

    def pick(hits):
        return jnp.where(hits, 1.0, 0.0)

    block = jnp.zeros_like(lane)
    for i, distance in enumerate(ring_order(n_hi)):
        block = jnp.where(lane // span_hi == i, (h + distance + n_hi) % n_hi, block)
    wanted = (lane % span_hi) * n_hi + block
    source = jnp.zeros_like(lane)
    target = jnp.zeros_like(lane)
    for i in range(orders.shape[1]):
        source = source + (((wanted >> orders[0, i]) & 1) << i)
        target = target + (((lane >> i) & 1) << orders[1, i])
    rows_one = pick(row == source).astype(BF16)
    p_out = lane // n_hi
    place_out = ((p_out // part_p) ^ c) * part_p + p_out % part_p
    out_one = pick((row[:span_hi] == place_out) & (lane % n_hi == h))
    out_one_bf = out_one.astype(BF16)
    rows_two = pick(row[:span_lo] == target - l * span_lo).astype(BF16)
    out_two = pick(row == (l ^ (lane // span_lo)) * span_lo + lane % span_lo).astype(BF16)

    turn = 0
    for own in edges:
        for j in range(own.shape[0]):
            rows = slice(turn * span_hi, (turn + 1) * span_hi)
            for piece, ref in zip(split(gate_ref[own[j, 0]]), (one_high, one_low)):
                moved = dot(out_one_bf, piece, ((1,), (1,))).astype(BF16)
                ref[rows] = dot(moved, rows_one).astype(BF16)
            high, low = split(gate_ref[own[j, 1]])
            picked = dot(rows_two, high) + dot(rows_two, low)
            for z in range(closed):
                front = out_one * close_ref[own[j, 2], 0, z : z + 1]
                front = jnp.sum(front, axis=1, keepdims=True)
                front_ref[turn, z] = jnp.broadcast_to(front, (span_hi, span_lo))
                scaled = picked * close_ref[own[j, 2], 1, z : z + 1]
                for piece, ref in zip(split(scaled), (two_high, two_low)):
                    ref[turn, z * span_lo : (z + 1) * span_lo] = dot(piece, out_two).astype(BF16)
            turn += 1


def sections_kernel(n_data, *refs):
    n_groups = len(refs[:-8]) // n_data
    groups = [refs[i * n_data : (i + 1) * n_data] for i in range(n_groups)]
    one_high, one_low, two_high, two_low, front_ref, keep, near, over = refs[n_data * n_groups :]
    slices, closed, span_hi, span_lo = front_ref.shape
    part_p = keep.shape[1]
    highs = [[] for _ in range(slices)]
    lows = [[] for _ in range(slices)]
    first_high, first_low = one_high[...], one_low[...]
    for chunks in groups:
        for i in range(chunks[0].shape[0]):
            data = jnp.concatenate(
                [jnp.concatenate([p[i, z] for z in range(closed)], axis=1) for p in chunks], axis=0
            )
            high, low = split(data)
            one = dot(first_high, high) + dot(first_low, high) + dot(first_high, low)
            for s in range(slices):
                scaled = [
                    one[s * span_hi : (s + 1) * span_hi, z * span_lo : (z + 1) * span_lo]
                    * front_ref[s, z]
                    for z in range(closed)
                ]
                high, low = split(jnp.concatenate(scaled, axis=1))
                highs[s].append(high)
                lows[s].append(low)
    total = None
    for s in range(slices):
        high, low = jnp.concatenate(highs[s], axis=0), jnp.concatenate(lows[s], axis=0)
        term = dot(high, two_high[s]) + dot(low, two_high[s]) + dot(high, two_low[s])
        total = term if total is None else total + term
    for b in range(keep.shape[0]):
        for k, line in enumerate(((keep, near), (over.at[0], over.at[1]))):
            rows = slice(b * span_hi + k * part_p, b * span_hi + (k + 1) * part_p)
            for j, ref in enumerate(line):
                ref[b] = total[rows, j * span_lo : (j + 1) * span_lo]


def place_kernel(n_cuts, keep, near, over, far, out_ref):
    c = lax.axis_index("cuts")
    n_hi, part_p = keep.shape[:2]
    for b in range(n_hi):
        for k, total in enumerate((keep[b] + near[b], over[0, b] + far[b])):
            out_ref[pl.ds(b * n_cuts + (c ^ k), part_p, stride=n_hi * n_cuts), :] = total


def cost(flops, bytes_accessed):
    return pl.CostEstimate(flops=flops, bytes_accessed=bytes_accessed, transcendentals=0)


def ring(value, step):
    n = lax.axis_size("hi")
    return lax.ppermute(value, "hi", [(i, (i + step) % n) for i in range(n)])


def tiled(state_block, gate_table, closing_table, edges, bit_orders):
    n_hi, n_lo, n_cuts = lax.axis_size("hi"), lax.axis_size("lo"), lax.axis_size("cuts")
    gate = gate_table.shape[1]
    closed = closing_table.shape[2]
    span_hi, span_lo = gate // n_hi, gate // n_lo
    part_p = span_hi // n_cuts
    slices = sum(own.shape[0] for own in edges)

    rows = state_block.reshape(-1, span_lo)
    ahead, back = pl.pallas_call(
        functools.partial(pack_kernel, n_hi, closed, n_lo),
        out_shape=[pinned((n_hi // 2, closed, span_hi, span_lo))] * 2,
        in_specs=[VMEM],
        out_specs=[VMEM] * 2,
        cost_estimate=cost(0, 2 * rows.size * 4),
        compiler_params=LIMIT,
        name="pack",
    )(rows)
    first, second = [ahead], [back]
    up, down = (ahead, back), (ahead, back)
    for t in range(1, n_hi // 2):
        up_ahead, down_back = ring(up[0], 1), ring(down[1], -1)
        up = (up_ahead, ring(up[1], 1))
        down = (ring(down[0], -1), down_back)
        first += [up[0], down[0]]
        second += [up[1], down[1]]
    first.append(ring(up[0], 1))
    second.append(ring(down[1], -1))

    gates = pl.pallas_call(
        functools.partial(gates_kernel, n_hi, n_cuts),
        out_shape=[pinned((slices * span_hi, gate), BF16)] * 2
        + [pinned((slices, closed * span_lo, gate), BF16)] * 2
        + [pinned((slices, closed, span_hi, span_lo))],
        in_specs=[SMEM] * n_cuts + [SMEM, VMEM, VMEM],
        out_specs=[VMEM] * 5,
        cost_estimate=cost(2_000_000_000, 4_000_000),
        compiler_params=LIMIT,
        name="gates",
    )(*edges, bit_orders, gate_table, closing_table)

    quarter = (n_hi, part_p, span_lo)
    keep, near, over = pl.pallas_call(
        functools.partial(sections_kernel, n_hi),
        out_shape=[pinned(quarter), pinned(quarter), pinned((n_lo,) + quarter)],
        in_specs=[VMEM] * (2 * n_hi + 5),
        out_specs=[VMEM] * 3,
        cost_estimate=cost(1_600_000_000, 4_000_000),
        compiler_params=LIMIT,
        name="sections",
    )(*[held(value) for value in (*first, *second, *gates)])
    over = swap(over, "cuts", 1)
    near = swap(near, "lo", 1)
    far = swap(over[1], "lo", 1)
    out = pl.pallas_call(
        functools.partial(place_kernel, n_cuts),
        out_shape=jax.ShapeDtypeStruct((part_p * n_hi * n_lo, span_lo), F32),
        in_specs=[VMEM] * 4,
        out_specs=VMEM,
        cost_estimate=cost(0, 2 * part_p * gate * n_lo * 4),
        compiler_params=LIMIT,
        name="place",
    )(*[held(value) for value in (keep, near, over, far)])
    return out.reshape(1, 1, -1)


def local(state_block, gate_table, closing_table, slice_edges, bit_orders):
    n_hi, n_lo, n_cuts = lax.axis_size("hi"), lax.axis_size("lo"), lax.axis_size("cuts")
    gate, closed = gate_table.shape[1], closing_table.shape[2]
    edges = [swap(slice_edges, "cuts", k) for k in range(n_cuts)]
    middle = state_block.shape[2] // (gate * gate * closed)
    whole = middle == 1 and n_lo == n_cuts == 2 and n_hi % 2 == 0 and gate // n_lo % 128 == 0
    if whole and gate // n_hi // n_cuts % 16 == 0:
        return tiled(state_block, gate_table, closing_table, edges, bit_orders)
    edges = jnp.concatenate(edges)
    return general(state_block, gate_table, closing_table, edges, bit_orders)


def solution(mesh):
    in_specs = (P(("group", "hi"), "lo", None), P(), P(), P(("group", "cuts"), None), P())
    out_specs = P(("group", "hi"), "lo", "cuts")
    return jax.shard_map(local, mesh=mesh, in_specs=in_specs, out_specs=out_specs, check_vma=False)
```

```python
import functools

import jax
import jax.numpy as jnp
from jax import lax
from jax.experimental import pallas as pl
from jax.experimental.pallas import tpu as pltpu
from jax.sharding import PartitionSpec as P

F32, BF16 = jnp.float32, jnp.bfloat16
VMEM = pl.BlockSpec(memory_space=pltpu.VMEM)
SMEM = pl.BlockSpec(memory_space=pltpu.SMEM)
LIMIT = pltpu.CompilerParams(vmem_limit_bytes=16 * 2**20)


def swap(value, axis, offset):
    if offset == 0:
        return value
    return lax.ppermute(value, axis, [(i, i ^ offset) for i in range(lax.axis_size(axis))])


def sources(order, wanted):
    total = jnp.zeros_like(wanted)
    for i in range(order.shape[0]):
        total = total + (((wanted >> order[i]) & 1) << i)
    return total


def general(state_block, gate_table, closing_table, edges, bit_orders):
    n_hi, n_lo, n_cuts = lax.axis_size("hi"), lax.axis_size("lo"), lax.axis_size("cuts")
    h, l, c = lax.axis_index("hi"), lax.axis_index("lo"), lax.axis_index("cuts")
    gate = gate_table.shape[1]
    closed = closing_table.shape[2]
    span_hi, span_lo = gate // n_hi, gate // n_lo
    middle = state_block.shape[2] // (gate * gate * closed)
    part_e = n_lo // n_cuts
    part_p = span_hi // n_cuts
    slices = edges.shape[0]

    view = state_block.reshape(span_hi, n_hi, closed, middle, n_cuts, part_e, span_lo)
    mine = lax.dynamic_index_in_dim(view, c, 4, keepdims=False)
    parts = []
    for d in range(n_hi):
        piece = lax.dynamic_index_in_dim(mine, h ^ d, 1, keepdims=False)
        parts.append(swap(piece, "hi", d))
    data = jnp.stack(parts).reshape(gate, closed, middle * part_e, span_lo)

    along = jnp.arange(gate, dtype=jnp.int32)
    in_rows = (along % span_hi) * n_hi + (h ^ (along // span_hi))
    out_p = (c ^ (along // part_p % n_cuts)) * part_p + along % part_p
    out_rows = out_p * n_hi + (h ^ (along // span_hi))
    in_cols = l * span_lo + jnp.arange(span_lo, dtype=jnp.int32)
    out_cols = (l ^ (along // span_lo)) * span_lo + along % span_lo
    rows_one = sources(bit_orders[0], in_rows)
    rows_two = sources(bit_orders[1], in_cols)
    firsts, seconds, fronts = [], [], []
    for s in range(slices):
        first = gate_table[edges[s, 0]]
        firsts.append(first[rows_one][:, out_rows].T)
        second = gate_table[edges[s, 1]][rows_two][:, out_cols]
        rear = closing_table[edges[s, 2], 1][:, out_cols]
        seconds.append(rear[:, None, :] * second[None])
        fronts.append(closing_table[edges[s, 2], 0][:, out_rows])
    first = jnp.stack(firsts).reshape(slices, n_hi, n_cuts, part_p, gate)
    front = jnp.stack(fronts).reshape(slices, closed, n_hi, n_cuts, part_p)
    second = jnp.stack(seconds)

    def sections(k):
        one = jnp.einsum(
            "sdpm,mzeq->sdpzeq", first[:, :, k], data, precision=lax.Precision.HIGH,
            preferred_element_type=F32,
        )
        one = one * jnp.transpose(front[:, :, :, k], (0, 2, 3, 1))[..., None, None]
        return jnp.einsum(
            "sdpzeq,szqn->depn", one, second, precision=lax.Precision.HIGH,
            preferred_element_type=F32,
        )

    others = [swap(sections(k), "cuts", k) for k in range(n_cuts)]
    both = jnp.stack(others).reshape(n_cuts, n_hi, middle * part_e, part_p, n_lo, span_lo)
    summed = sum(swap(both[:, :, :, :, k], "lo", k) for k in range(n_lo))
    out = jnp.zeros((part_p, n_hi, middle, n_cuts, part_e, span_lo), F32)
    for d in range(n_hi):
        piece = swap(summed[:, d], "hi", d).reshape(n_cuts, middle, part_e, part_p, span_lo)
        for k in range(n_cuts):
            block = jnp.transpose(piece[k], (2, 0, 1, 3))[:, None, :, None]
            out = lax.dynamic_update_slice(out, block, (0, h ^ d, 0, c ^ k, 0, 0))
    return out.reshape(1, 1, -1)


def split(value):
    high = value.astype(BF16)
    return high, (value - high.astype(F32)).astype(BF16)


def dot(a, b, sides=((1,), (0,))):
    return lax.dot_general(a, b, (sides, ((), ())), preferred_element_type=F32)


def pinned(shape, dtype=F32):
    return pltpu.VMEM(shape, dtype)


def held(value):
    return pltpu.with_memory_space_constraint(value, pltpu.VMEM)


def pack_kernel(closed, n_lo, x_ref, *pieces):
    h, c = lax.axis_index("hi"), lax.axis_index("cuts")
    n_hi, span = len(pieces), pieces[0].shape[1]
    for d, piece in enumerate(pieces):
        for z in range(closed):
            first = ((h ^ d) * closed + z) * n_lo + c
            piece[z] = x_ref[pl.ds(first, span, stride=n_hi * closed * n_lo), :]


def gates_kernel(n_hi, n_cuts, *refs):
    edges, (orders, gate_ref, close_ref) = refs[:n_cuts], refs[n_cuts : n_cuts + 3]
    one_high, one_low, two_high, two_low, front_ref = refs[n_cuts + 3 :]
    h, l, c = (lax.axis_index(name) for name in ("hi", "lo", "cuts"))
    gate = gate_ref.shape[1]
    closed, span_lo = front_ref.shape[1], front_ref.shape[3]
    span_hi = gate // n_hi
    part_p = span_hi // n_cuts
    lane = lax.broadcasted_iota(jnp.int32, (1, gate), 1)
    row = lax.broadcasted_iota(jnp.int32, (gate, gate), 0)

    def pick(hits):
        return jnp.where(hits, 1.0, 0.0)

    wanted = (lane % span_hi) * n_hi + (h ^ (lane // span_hi))
    source = jnp.zeros_like(lane)
    target = jnp.zeros_like(lane)
    for i in range(orders.shape[1]):
        source = source + (((wanted >> orders[0, i]) & 1) << i)
        target = target + (((lane >> i) & 1) << orders[1, i])
    rows_one = pick(row == source).astype(BF16)
    p_out = lane // n_hi
    place_out = ((lane % n_hi) ^ h) * span_hi + ((p_out // part_p) ^ c) * part_p + p_out % part_p
    out_one = pick(row == place_out)
    out_one_bf = out_one.astype(BF16)
    rows_two = pick(row[:span_lo] == target - l * span_lo).astype(BF16)
    out_two = pick(row == (l ^ (lane // span_lo)) * span_lo + lane % span_lo).astype(BF16)

    turn = 0
    for own in edges:
        for j in range(own.shape[0]):
            rows = slice(turn * gate, (turn + 1) * gate)
            for piece, ref in zip(split(gate_ref[own[j, 0]]), (one_high, one_low)):
                moved = dot(out_one_bf, piece, ((1,), (1,))).astype(BF16)
                ref[rows] = dot(moved, rows_one).astype(BF16)
            high, low = split(gate_ref[own[j, 1]])
            picked = dot(rows_two, high) + dot(rows_two, low)
            for z in range(closed):
                front = out_one * close_ref[own[j, 2], 0, z : z + 1]
                front = jnp.sum(front, axis=1, keepdims=True)
                front_ref[turn, z] = jnp.broadcast_to(front, (gate, span_lo))
                scaled = picked * close_ref[own[j, 2], 1, z : z + 1]
                for piece, ref in zip(split(scaled), (two_high, two_low)):
                    ref[turn, z * span_lo : (z + 1) * span_lo] = dot(piece, out_two).astype(BF16)
            turn += 1


def sections_kernel(*refs):
    pieces = refs[:-8]
    one_high, one_low, two_high, two_low, front_ref, keep, near, over = refs[-8:]
    slices, closed, gate, span_lo = front_ref.shape
    n_hi, part_p = keep.shape[:2]
    data = jnp.concatenate(
        [jnp.concatenate([p[z] for z in range(closed)], axis=1) for p in pieces], axis=0
    )
    data_high, data_low = split(data)
    total = None
    for s in range(slices):
        rows = slice(s * gate, (s + 1) * gate)
        first = one_high[rows]
        one = dot(first, data_high) + dot(one_low[rows], data_high) + dot(first, data_low)
        scaled = [
            one[:, z * span_lo : (z + 1) * span_lo] * front_ref[s, z] for z in range(closed)
        ]
        high, low = split(jnp.concatenate(scaled, axis=1))
        term = dot(high, two_high[s]) + dot(low, two_high[s]) + dot(high, two_low[s])
        total = term if total is None else total + term
    for d in range(n_hi):
        for k, line in enumerate(((keep, near), (over.at[0], over.at[1]))):
            rows = slice((d * 2 + k) * part_p, (d * 2 + k + 1) * part_p)
            for j, ref in enumerate(line):
                ref[d] = total[rows, j * span_lo : (j + 1) * span_lo]


def merge_kernel(keep, near, over, far, *ends):
    for d, end in enumerate(ends):
        end[0] = keep[d] + near[d]
        end[1] = over[0, d] + far[d]


def place_kernel(*refs):
    h, c = lax.axis_index("hi"), lax.axis_index("cuts")
    ends, out_ref = refs[:-1], refs[-1]
    n_cuts, part_p = ends[0].shape[:2]
    for d, end in enumerate(ends):
        for k in range(n_cuts):
            first = (h ^ d) * n_cuts + (c ^ k)
            out_ref[pl.ds(first, part_p, stride=len(ends) * n_cuts), :] = end[k]


def cost(flops, bytes_accessed):
    return pl.CostEstimate(flops=flops, bytes_accessed=bytes_accessed, transcendentals=0)


def tiled(state_block, gate_table, closing_table, edges, bit_orders):
    n_hi, n_lo, n_cuts = lax.axis_size("hi"), lax.axis_size("lo"), lax.axis_size("cuts")
    gate = gate_table.shape[1]
    closed = closing_table.shape[2]
    span_hi, span_lo = gate // n_hi, gate // n_lo
    part_p = span_hi // n_cuts
    slices = sum(own.shape[0] for own in edges)

    rows = state_block.reshape(-1, span_lo)
    pieces = pl.pallas_call(
        functools.partial(pack_kernel, closed, n_lo),
        out_shape=[pinned((closed, span_hi, span_lo))] * n_hi,
        in_specs=[VMEM],
        out_specs=[VMEM] * n_hi,
        cost_estimate=cost(0, 2 * rows.size * 4),
        compiler_params=LIMIT,
        name="pack",
    )(rows)
    data = []
    for d, piece in enumerate(pieces):
        with jax.named_scope(f"in{d}"):
            data.append(swap(piece, "hi", d))

    gates = pl.pallas_call(
        functools.partial(gates_kernel, n_hi, n_cuts),
        out_shape=[pinned((slices * gate, gate), BF16)] * 2
        + [pinned((slices, closed * span_lo, gate), BF16)] * 2
        + [pinned((slices, closed, gate, span_lo))],
        in_specs=[SMEM] * n_cuts + [SMEM, VMEM, VMEM],
        out_specs=[VMEM] * 5,
        cost_estimate=cost(2_000_000_000, 4_000_000),
        compiler_params=LIMIT,
        name="gates",
    )(*edges, bit_orders, gate_table, closing_table)

    quarter = (n_hi, part_p, span_lo)
    keep, near, over = pl.pallas_call(
        sections_kernel,
        out_shape=[pinned(quarter), pinned(quarter), pinned((n_lo,) + quarter)],
        in_specs=[VMEM] * (n_hi + 5),
        out_specs=[VMEM] * 3,
        cost_estimate=cost(1_600_000_000, 4_000_000),
        compiler_params=LIMIT,
        name="sections",
    )(*[held(value) for value in (*data, *gates)])
    over = swap(over, "cuts", 1)
    near = swap(near, "lo", 1)
    far = swap(over[1], "lo", 1)
    ends = pl.pallas_call(
        merge_kernel,
        out_shape=[pinned((n_cuts, part_p, span_lo))] * n_hi,
        in_specs=[VMEM] * 4,
        out_specs=[VMEM] * n_hi,
        cost_estimate=cost(0, 2_000_000),
        compiler_params=LIMIT,
        name="merge",
    )(*[held(value) for value in (keep, near, over, far)])
    placed = []
    for d, end in enumerate(ends):
        with jax.named_scope(f"out{d}"):
            placed.append(swap(end, "hi", d))
    out = pl.pallas_call(
        place_kernel,
        out_shape=jax.ShapeDtypeStruct((part_p * n_hi * n_lo, span_lo), F32),
        in_specs=[VMEM] * n_hi,
        out_specs=VMEM,
        cost_estimate=cost(0, 2 * part_p * gate * n_lo * 4),
        compiler_params=LIMIT,
        name="place",
    )(*[held(value) for value in placed])
    return out.reshape(1, 1, -1)


def local(state_block, gate_table, closing_table, slice_edges, bit_orders):
    n_hi, n_lo, n_cuts = lax.axis_size("hi"), lax.axis_size("lo"), lax.axis_size("cuts")
    gate, closed = gate_table.shape[1], closing_table.shape[2]
    edges = [swap(slice_edges, "cuts", k) for k in range(n_cuts)]
    middle = state_block.shape[2] // (gate * gate * closed)
    whole = middle == 1 and n_lo == n_cuts == 2 and gate // n_lo % 128 == 0
    if whole and gate // n_hi // n_cuts % 16 == 0:
        return tiled(state_block, gate_table, closing_table, edges, bit_orders)
    edges = jnp.concatenate(edges)
    return general(state_block, gate_table, closing_table, edges, bit_orders)


def solution(mesh):
    in_specs = (P(("group", "hi"), "lo", None), P(), P(), P(("group", "cuts"), None), P())
    out_specs = P(("group", "hi"), "lo", "cuts")
    return jax.shard_map(local, mesh=mesh, in_specs=in_specs, out_specs=out_specs, check_vma=False)
```
